256 devices in a mesh: row: 8 (over y_lo, x), col: 32 (over z, y_hi, core).
Axes of the slice: x: 4, y: 4 (y_hi: 2, y_lo: 2; y = y_hi * 2 + y_lo), z: 8, core: 2. Of those that a mesh axis runs over, the one named last changes fastest.
Arguments:
- charge: float32 [256, 256, 256], P('col', 'row'), may hold values from -6 to 6
- green_spectrum: float32 [512, 512, 512], P('row', 'col'), may hold values from 0.2 to 2
Outputs:
- potential: float32 [256, 256, 256], P('col', 'row')
The draws below stay inside these ranges and needn't reach their ends.
All inputs are finite; a program needn't handle non-finite values.
Results may differ from the reference program's by a relative error of at most 0.00007.
Values sent between devices are 32-bit elements; how exact they have to be, the bound alone decides.
No kernel may reach another device: no remote copies, remote signals or barrier semaphores. Data moves between devices by JAX's collectives and lax.ppermute only.
A program may use at most 128 MiB of HBM per device.

```python
import math
import jax
import jax.numpy as jnp

M = 512
N = 256


def block_levels(key, shape, shards, low, largest):
    gain, own = 1.0, jax.random.fold_in(key, 6)
    for axis_at, blocks in shards:
        heights = jnp.exp(jax.random.uniform(jax.random.fold_in(own, axis_at), (blocks,), jnp.float32, low / len(shards), largest / len(shards)))
        gain = gain * jnp.repeat(heights, shape[axis_at] // blocks).reshape([-1 if axis == axis_at else 1 for axis in range(len(shape))])
    return gain


def noise(rng, dims, spread, bound, shards=(), held_as=jnp.bfloat16):
    array = jax.random.normal(rng, dims, jnp.float32) * spread
    if len(shards) > 0:
        array = block_levels(rng, dims, shards, -0.22, 0.18) * array
    return jnp.clip(array, min=-bound, max=bound).astype(held_as)


def setup_inputs(seed: int = 0) -> dict:
    seeds = jax.random.split(jax.random.key(seed), 3)
    charge = noise(seeds[0], (N, N, N), 1.0, 6.0, ((0, 32), (1, 8)), jnp.float32)
    green_spectrum = jnp.clip(jnp.exp(math.log(2.0) - 2.3025851 * jax.random.uniform(seeds[1], (M, M, M), jnp.float32) ** block_levels(seeds[1], (M, M, M), ((0, 8), (1, 32)), -0.2, 0.2)), 0.2, 2.0)
    return {"charge": charge, "green_spectrum": green_spectrum}


def reference(charge, green_spectrum):
    spectrum = jnp.fft.fft(charge, n=M, axis=2)
    spectrum = jnp.fft.fft(spectrum, n=M, axis=1)
    spectrum = jnp.fft.fft(spectrum, n=M, axis=0)
    product = spectrum * jnp.transpose(green_spectrum, (2, 1, 0))
    field = jnp.fft.ifft(product, axis=0)[:N]
    field = jnp.fft.ifft(field, axis=1)[:, :N]
    field = jnp.fft.ifft(field, axis=2)[:, :, :N]
    return jnp.real(field).astype(jnp.float32)
```

```python
import functools

import jax
import jax.numpy as jnp
import ml_dtypes
import numpy as np
from jax import lax
from jax.experimental import pallas as pl
from jax.experimental.pallas import tpu as pltpu
from jax.sharding import PartitionSpec as P

M = 512
N = 256
LANES = 128
HALF = 64
BF16 = jnp.bfloat16


def split_table(table):
    high = table.astype(ml_dtypes.bfloat16)
    low = (table - high.astype(np.float64)).astype(ml_dtypes.bfloat16)
    return high, low


@functools.cache
def tables():
    freq = np.arange(M)[:, None]
    cell = np.arange(N)[None, :]
    angle = 2.0 * np.pi * ((freq * cell) % M) / M
    cosine, sine = np.cos(angle), np.sin(angle)
    forward = np.concatenate([cosine, sine], 1)
    backward = np.concatenate([cosine.T, sine.T], 0)
    return split_table(forward) + split_table(backward)


def halves(value):
    high = value.astype(BF16)
    low = (value - high.astype(jnp.float32)).astype(BF16)
    return high, low


def mul(left, right, dims=((1,), (0,))):
    dot = functools.partial(
        lax.dot_general, dimension_numbers=(dims, ((), ())), preferred_element_type=jnp.float32
    )
    (lh, ll), (rh, rl) = left, right
    return dot(lh, rh) + (dot(lh, rl) + dot(ll, rh))


def swap_parts(value):
    return pltpu.roll(value, HALF, 1)


def real_lanes(shape):
    return lax.broadcasted_iota(jnp.int32, shape, 1) < HALF


def forward_rows(data):
    turned = swap_parts(data)
    turned = jnp.where(real_lanes(data.shape), turned, -turned)
    return jnp.concatenate([data, turned], 0)


def backward_join(both):
    n = both.shape[0] // 2
    even, odd = both[:n], swap_parts(both[n:])
    return even + jnp.where(real_lanes(odd.shape), -odd, odd)


def z_rows(table, r):
    rows = slice(HALF * r, HALF * (r + 1))
    return jnp.concatenate([table[rows, :N], -table[rows, N:]], 0)


def z_forward(charge, th, tl, out):
    value = halves(charge[...])
    for r in range(out.shape[0]):
        out[r] = mul(value, (z_rows(th, r), z_rows(tl, r)), ((1,), (1,)))


def y_forward(data, th, tl, out):
    table = (th[...], tl[...])

    def step(k, carry):
        cols = [
            forward_rows(data[:, 2 * k + i].reshape(N, LANES)) for i in range(2)
        ]
        both = mul(table, halves(jnp.concatenate(cols, 1)))
        for i in range(2):
            out[:, 2 * k + i] = both[:, LANES * i : LANES * (i + 1)].reshape(32, 16, LANES)
        return carry

    lax.fori_loop(0, 4, step, 0)


def x_both(data, green, fh, fl, bh, bl, out):
    forward = (fh[...], fl[...])
    backward = (bh[...], bl[...])

    def step(k, carry):
        cols = [
            forward_rows(data[pl.ds(2 * k + i, N, stride=16), :]) for i in range(2)
        ]
        spectrum = mul(forward, halves(jnp.concatenate(cols, 1)))
        product = spectrum * jnp.concatenate([green[2 * k + i] for i in range(2)], 1)
        both = mul(backward, halves(product))
        for i in range(2):
            field = backward_join(both[:, LANES * i : LANES * (i + 1)])
            out[:, 2 * k + i] = field.reshape(32, 8, LANES)
        return carry

    lax.fori_loop(0, 8, step, 0)


def y_backward(data, bh, bl, out):
    backward = (bh[...], bl[...])

    def step(k, carry):
        cols = [data[pl.ds(2 * k + i, M, stride=8), :] for i in range(2)]
        both = mul(backward, halves(jnp.concatenate(cols, 1)))
        for i in range(2):
            field = backward_join(both[:, LANES * i : LANES * (i + 1)])
            out[:, 2 * k + i] = field.reshape(8, 32, LANES)
        return carry

    lax.fori_loop(0, 4, step, 0)


def z_backward(data, th, tl, out):
    total = 0.0
    for r in range(data.shape[0]):
        total += mul(halves(data[r]), (z_rows(th, r), z_rows(tl, r)))
    out[...] = total * (1.0 / M**3)


def turn_green(green, out):
    for b in range(16):
        part = green[:, b, :]
        out[b] = jnp.concatenate([part, part], 0).T


def call(body, shape, flops, *args):
    return pl.pallas_call(
        body,
        out_shape=jax.ShapeDtypeStruct(shape, jnp.float32),
        in_specs=[pl.BlockSpec(memory_space=pltpu.VMEM)] * len(args),
        out_specs=pl.BlockSpec(memory_space=pltpu.VMEM),
        compiler_params=pltpu.CompilerParams(vmem_limit_bytes=48 * 1024 * 1024),
        cost_estimate=pl.CostEstimate(
            flops=flops, bytes_accessed=4 * int(np.prod(shape)), transcendentals=0
        ),
        name=body.__name__,
    )(*args)


def exchange(value, axis):
    return lax.all_to_all(value, axis, split_axis=0, concat_axis=0, tiled=True)


def on_device(charge, green_spectrum):
    fh, fl, bh, bl = (jnp.asarray(t) for t in tables())
    green = call(turn_green, (16, M, LANES), 10**9, green_spectrum)
    along_z = call(z_forward, (8, 256, LANES), 10**9, charge.reshape(256, N), fh, fl)
    by_rows = exchange(along_z, "row")
    along_y = call(
        y_forward, (32, 8, 16, LANES), 10**9, by_rows.reshape(8, 8, 32, LANES), fh, fl
    )
    by_cols = exchange(along_y.reshape(32, LANES, LANES), "col")
    back_x = call(
        x_both, (32, 16, 8, LANES), 10**9, by_cols.reshape(4096, LANES), green, fh, fl, bh, bl
    )
    by_cells = exchange(back_x.reshape(32, LANES, LANES), "col")
    back_y = call(
        y_backward, (8, 8, 32, LANES), 10**9, by_cells.reshape(4096, LANES), bh, bl
    )
    by_parts = exchange(back_y.reshape(8, 256, LANES), "row")
    back_z = call(z_backward, (256, N), 10**9, by_parts, fh, fl)
    return back_z.reshape(8, 32, N)


def solution(mesh):
    in_specs = (P("col", "row", None), P("row", "col", None))
    out_specs = P("col", "row", None)
    return jax.shard_map(
        on_device, mesh=mesh, in_specs=in_specs, out_specs=out_specs, check_vma=False
    )
```

```python
import functools

import jax
import jax.numpy as jnp
import ml_dtypes
import numpy as np
from jax import lax
from jax.experimental import pallas as pl
from jax.experimental.pallas import tpu as pltpu
from jax.sharding import PartitionSpec as P

M = 512
N = 256
LANES = 128
HALF = 64
BF16 = jnp.bfloat16


def split_table(table):
    high = table.astype(ml_dtypes.bfloat16)
    low = (table - high.astype(np.float64)).astype(ml_dtypes.bfloat16)
    return high, low


@functools.cache
def tables():
    freq = np.arange(N)[:, None]
    pair = np.arange(N // 2)[None, :]
    forward = []
    for parity in range(2):
        angle = 2.0 * np.pi * ((freq * (2 * pair + parity)) % M) / M
        forward.append(np.concatenate([np.cos(angle), np.sin(angle)], 1))
    forward = np.stack(forward)
    angle = 2.0 * np.pi * ((np.arange(M)[:, None] * np.arange(N)[None, :]) % M) / M
    angle = angle.reshape(8, HALF, N)
    along_z = np.concatenate([np.cos(angle), -np.sin(angle)], 1).reshape(2 * M, N)
    return tuple(
        np.stack(split_table(t)) for t in (along_z, forward, forward.transpose(0, 2, 1))
    )


def halves(value):
    high = value.astype(BF16)
    low = (value - high.astype(jnp.float32)).astype(BF16)
    return high, low


def mul(left, right, dims=((1,), (0,))):
    dot = functools.partial(
        lax.dot_general, dimension_numbers=(dims, ((), ())), preferred_element_type=jnp.float32
    )
    (lh, ll), (rh, rl) = left, right
    return dot(lh, rh) + (dot(lh, rl) + dot(ll, rh))


def swap_parts(value):
    return pltpu.roll(value, HALF, 1)


def real_lanes(shape):
    return lax.broadcasted_iota(jnp.int32, shape, 1) < HALF


def forward_rows(data):
    turned = swap_parts(data)
    turned = jnp.where(real_lanes(data.shape), turned, -turned)
    return jnp.concatenate([data, turned], 0)


def backward_join(both):
    n = both.shape[0] // 2
    even, odd = both[:n], swap_parts(both[n:])
    return even + jnp.where(real_lanes(odd.shape), -odd, odd)


def z_forward(charge, table, out):
    value = halves(charge[...])
    for r in range(out.shape[0]):
        rows = slice(LANES * r, LANES * (r + 1))
        out[r] = mul(value, (table[0, rows], table[1, rows]), ((1,), (1,)))


def both_parities(table, cols):
    return [
        mul((table[0, p], table[1, p]), halves(jnp.concatenate([forward_rows(c) for c in cols[p]], 1)))
        for p in range(2)
    ]


def y_forward(data, table, out):
    def step(k, carry):
        cols = [
            [
                jnp.concatenate(
                    [data[pl.ds(256 * s + 32 * (2 * k + i) + p, 16, stride=2), :] for s in range(8)], 0
                )
                for i in range(2)
            ]
            for p in range(2)
        ]
        even, odd = both_parities(table, cols)
        for i in range(2):
            at = slice(LANES * i, LANES * (i + 1))
            low, high = even[:, at] + odd[:, at], even[:, at] - odd[:, at]
            out[:16, 2 * k + i] = low.reshape(16, 16, LANES)
            out[16:, 2 * k + i] = high.reshape(16, 16, LANES)
        return carry

    lax.fori_loop(0, 4, step, 0, unroll=2)


def x_both(data, green, forward, backward, out):
    def step(k, carry):
        cols = [
            [data[pl.ds(16 * p + 2 * k + i, LANES, stride=32), :] for i in range(2)]
            for p in range(2)
        ]
        even, odd = both_parities(forward, cols)
        low, high = (
            jnp.concatenate([green[2 * k + i, N * h : N * (h + 1)] for i in range(2)], 1)
            for h in range(2)
        )
        low, high = (even + odd) * low, (even - odd) * high
        for p, value in enumerate((low + high, low - high)):
            both = mul((backward[0, p], backward[1, p]), halves(value))
            for i in range(2):
                field = backward_join(both[:, LANES * i : LANES * (i + 1)])
                out[pl.ds(16 * p + 2 * k + i, LANES, stride=32), :] = field
        return carry

    lax.fori_loop(0, 8, step, 0, unroll=2)


def y_backward(data, backward, out):
    def step(k, carry):
        low, high = (
            jnp.concatenate(
                [data[16 * h : 16 * (h + 1), 2 * k + i].reshape(N, LANES) for i in range(2)], 1
            )
            for h in range(2)
        )
        for p, value in enumerate((low + high, low - high)):
            both = mul((backward[0, p], backward[1, p]), halves(value))
            for i in range(2):
                field = backward_join(both[:, LANES * i : LANES * (i + 1)])
                for s in range(8):
                    rows = pl.ds(256 * s + 32 * (2 * k + i) + p, 16, stride=2)
                    out[rows, :] = field[16 * s : 16 * (s + 1)]
        return carry

    lax.fori_loop(0, 4, step, 0, unroll=2)


def z_backward(data, table, out):
    total = 0.0
    for r in range(data.shape[0]):
        rows = slice(LANES * r, LANES * (r + 1))
        total += mul(halves(data[r]), (table[0, rows], table[1, rows]))
    out[...] = total * (1.0 / M**3)


def turn_green(green, out):
    for b in range(16):
        part = green[:, b, :]
        out[b] = jnp.concatenate([part, part], 0).T


def call(body, shape, grant, *args):
    return pl.pallas_call(
        body,
        out_shape=jax.ShapeDtypeStruct(shape, jnp.float32),
        in_specs=[pl.BlockSpec(memory_space=pltpu.VMEM)] * len(args),
        out_specs=pl.BlockSpec(memory_space=pltpu.VMEM),
        compiler_params=pltpu.CompilerParams(vmem_limit_bytes=grant * 1024 * 1024),
        cost_estimate=pl.CostEstimate(
            flops=10**9, bytes_accessed=4 * int(np.prod(shape)), transcendentals=0
        ),
        name=body.__name__,
    )(*args)


def exchange(value, axis):
    return lax.all_to_all(value, axis, split_axis=0, concat_axis=0, tiled=True)


def on_device(charge, green_spectrum):
    z_table, forward, backward = (jnp.asarray(t) for t in tables())
    green = call(turn_green, (16, M, LANES), 60, green_spectrum)
    along_z = call(z_forward, (8, 256, LANES), 60, charge.reshape(256, N), z_table)
    by_rows = exchange(along_z, "row").reshape(2048, LANES)
    along_y = call(y_forward, (32, 8, 16, LANES), 60, by_rows, forward)
    by_cols = exchange(along_y.reshape(32, LANES, LANES), "col").reshape(4096, LANES)
    back_x = call(x_both, (4096, LANES), 16, by_cols, green, forward, backward)
    by_cells = exchange(back_x.reshape(32, LANES, LANES), "col")
    back_y = call(
        y_backward, (2048, LANES), 16, by_cells.reshape(32, 8, 16, LANES), backward
    )
    by_parts = exchange(back_y.reshape(8, 256, LANES), "row")
    back_z = call(z_backward, (256, N), 16, by_parts, z_table)
    return back_z.reshape(8, 32, N)


def solution(mesh):
    in_specs = (P("col", "row", None), P("row", "col", None))
    out_specs = P("col", "row", None)
    return jax.shard_map(
        on_device, mesh=mesh, in_specs=in_specs, out_specs=out_specs, check_vma=False
    )
```

```python
import functools

import jax
import jax.numpy as jnp
import ml_dtypes
import numpy as np
from jax import lax
from jax.experimental import pallas as pl
from jax.experimental.pallas import tpu as pltpu
from jax.sharding import PartitionSpec as P

M = 512
N = 256
LANES = 128
HALF = 64
SLOTS = 32
BF16 = jnp.bfloat16


def split_table(table):
    high = table.astype(ml_dtypes.bfloat16)
    low = (table - high.astype(np.float64)).astype(ml_dtypes.bfloat16)
    return high, low


@functools.cache
def tables():
    freq = np.arange(N)[:, None]
    pair = np.arange(N // 2)[None, :]
    forward = []
    for parity in range(2):
        angle = 2.0 * np.pi * ((freq * (2 * pair + parity)) % M) / M
        forward.append(np.concatenate([np.cos(angle), np.sin(angle)], 1))
    forward = np.stack(forward)
    freq = np.arange(8)[:, None] * HALF + np.arange(SLOTS)[None, :]
    freq[:4, 0] += SLOTS
    angle = 2.0 * np.pi * ((freq[:, :, None] * np.arange(N)) % M) / M
    back_z = np.concatenate([np.cos(angle), -np.sin(angle)], 1).reshape(M, N)
    own = np.concatenate([freq == N, freq == N], 1).reshape(M, 1)
    along_z = np.where(own, 0.5, 1.0) * back_z
    return tuple(
        np.stack(split_table(t)) for t in (along_z, back_z, forward, forward.transpose(0, 2, 1))
    )


def halves(value):
    high = value.astype(BF16)
    low = (value - high.astype(jnp.float32)).astype(BF16)
    return high, low


def mul(left, right, dims=((1,), (0,))):
    dot = functools.partial(
        lax.dot_general, dimension_numbers=(dims, ((), ())), preferred_element_type=jnp.float32
    )
    (lh, ll), (rh, rl) = left, right
    return dot(lh, rh) + (dot(lh, rl) + dot(ll, rh))


def real_lanes(value):
    return lax.broadcasted_iota(jnp.int32, value.shape, 1) % HALF < SLOTS


def forward_rows(data):
    after, before = pltpu.roll(data, LANES - SLOTS, 1), pltpu.roll(data, SLOTS, 1)
    return jnp.concatenate([data, jnp.where(real_lanes(data), after, -before)], 0)


def backward_join(both):
    n = both.shape[0] // 2
    sine = both[n:]
    after, before = pltpu.roll(sine, LANES - SLOTS, 1), pltpu.roll(sine, SLOTS, 1)
    return both[:n] + jnp.where(real_lanes(sine), -after, before)


def trade(first, second):
    low = lax.broadcasted_iota(jnp.int32, first.shape, 1) < HALF
    turned = [pltpu.roll(v, HALF, 1) for v in (first, second)]
    return jnp.where(low, first, turned[1]), jnp.where(low, turned[0], second)


def z_forward(charge, table, out):
    value = halves(charge[...])
    for q in range(4):
        rows = slice(LANES * q, LANES * (q + 1))
        pair = mul(value, (table[0, rows], table[1, rows]), ((1,), (1,)))
        out[2 * q], out[2 * q + 1] = trade(pair[:LANES], pair[LANES:])


def both_parities(table, cols):
    return [
        mul((table[0, p], table[1, p]), halves(jnp.concatenate([forward_rows(c) for c in cols[p]], 1)))
        for p in range(2)
    ]


def y_forward(data, table, out):
    for k in range(2):
        cols = [
            [
                jnp.concatenate(
                    [data[pl.ds(128 * s + 32 * (2 * k + i) + p, 16, stride=2), :] for s in range(8)], 0
                )
                for i in range(2)
            ]
            for p in range(2)
        ]
        even, odd = both_parities(table, cols)
        for i in range(2):
            at = slice(LANES * i, LANES * (i + 1))
            for h, value in enumerate((even[:, at] + odd[:, at], even[:, at] - odd[:, at])):
                value = value.reshape(16, 2, 8, LANES)
                pair = trade(value[:, 0].reshape(LANES, LANES), value[:, 1].reshape(LANES, LANES))
                for x in range(2):
                    out[16 * h : 16 * (h + 1), 4 * x + 2 * k + i] = pair[x].reshape(16, 8, LANES)


def x_both(data, green, forward, backward, out):
    def step(k, carry):
        cols = [
            [data[pl.ds(8 * p + 2 * k + i, LANES, stride=16), :] for i in range(2)]
            for p in range(2)
        ]
        even, odd = both_parities(forward, cols)
        low, high = (
            jnp.concatenate([green[2 * k + i, N * h : N * (h + 1)] for i in range(2)], 1)
            for h in range(2)
        )
        low, high = (even + odd) * low, (even - odd) * high
        for p, value in enumerate((low + high, low - high)):
            both = mul((backward[0, p], backward[1, p]), halves(value))
            for i in range(2):
                field = backward_join(both[:, LANES * i : LANES * (i + 1)])
                out[pl.ds(8 * p + 2 * k + i, LANES, stride=16), :] = field
        return carry

    lax.fori_loop(0, 4, step, 0, unroll=2)


def y_backward(data, backward, out):
    for k in range(2):
        low_high = []
        for h in range(2):
            part = []
            for i in range(2):
                pair = trade(
                    *(
                        data[16 * h : 16 * (h + 1), 4 * x + 2 * k + i].reshape(LANES, LANES)
                        for x in range(2)
                    )
                )
                part.append(
                    jnp.stack([v.reshape(16, 8, LANES) for v in pair], 1).reshape(N, LANES)
                )
            low_high.append(jnp.concatenate(part, 1))
        low, high = low_high
        for p, value in enumerate((low + high, low - high)):
            both = mul((backward[0, p], backward[1, p]), halves(value))
            for i in range(2):
                field = backward_join(both[:, LANES * i : LANES * (i + 1)])
                for s in range(8):
                    rows = pl.ds(128 * s + 32 * (2 * k + i) + p, 16, stride=2)
                    out[rows, :] = field[16 * s : 16 * (s + 1)]


def z_backward(data, table, out):
    total = 0.0
    for q in range(4):
        rows = slice(LANES * q, LANES * (q + 1))
        pair = jnp.concatenate(trade(data[2 * q], data[2 * q + 1]), 0)
        total += mul(halves(pair), (table[0, rows], table[1, rows]))
    out[...] = total * (1.0 / M**3)


def turn_green(late, green, mirror, mirror_edge, start, start_edge, zero, out):
    late = late[0] == 1
    slot = lax.broadcasted_iota(jnp.int32, (SLOTS, M), 0)
    sign = jnp.where(slot % 2 == 1, 1.0, -1.0)
    row, col = (lax.broadcasted_iota(jnp.int32, (M, M), d) for d in range(2))
    swap = jnp.where((row + col) % M == 0, 1.0, 0.0).astype(BF16)
    row, col = (lax.broadcasted_iota(jnp.int32, (LANES, HALF), d) for d in range(2))
    same = (row // HALF == col // SLOTS) & ((row + col) % SLOTS == 0)
    turn = jnp.where(same, 1.0, 0.0).astype(BF16)
    dot = functools.partial(lax.dot_general, preferred_element_type=jnp.float32)
    nn, nt = (((1,), (0,)), ((), ())), (((1,), (1,)), ((), ()))

    def rows(array, at):
        return jnp.broadcast_to(array[at : at + 1, :], (SLOTS, M))

    for k in range(8):
        owns, others = [], []
        for b in (k, 8 + k):
            mid = jnp.broadcast_to(green[SLOTS, b : b + 1, :], (SLOTS, M))
            own = jnp.where((slot == 0) & ~late, mid, green[0:SLOTS, b, :])
            owns.append(own + sign * rows(zero, b))
            if b == 0:
                other, begin, nil = mirror_edge[...], rows(start_edge, 0), rows(zero, 32)
            else:
                other, begin, nil = mirror[:, 16 - b, :], rows(start, 16 - b), rows(zero, 32 - b)
            other = jnp.where((slot == 0) & late, begin, other)
            others.append(other + sign * nil)
        own = jnp.concatenate([owns[0], owns[0], owns[1], owns[1]], 0)
        oh, ol = halves(jnp.concatenate(others, 0))
        oh, ol = halves(dot(turn, oh, nn) + dot(turn, ol, nn))
        out[k] = own.T + (dot(swap, oh, nt) + dot(swap, ol, nt))


def call(body, shape, grant, *args, scalars=0):
    vmem, smem = (pl.BlockSpec(memory_space=m) for m in (pltpu.VMEM, pltpu.SMEM))
    return pl.pallas_call(
        body,
        out_shape=jax.ShapeDtypeStruct(shape, jnp.float32),
        in_specs=[smem] * scalars + [vmem] * (len(args) - scalars),
        out_specs=vmem,
        compiler_params=pltpu.CompilerParams(vmem_limit_bytes=grant * 1024 * 1024),
        cost_estimate=pl.CostEstimate(
            flops=10**9, bytes_accessed=4 * int(np.prod(shape)), transcendentals=0
        ),
        name=body.__name__,
    )(*args)


def exchange(value, axis):
    return lax.all_to_all(value, axis, split_axis=0, concat_axis=0, tiled=True)


def reflect(value, row_shift, col_shift):
    pairs = [
        (32 * r + j, 32 * ((row_shift - r) % 8) + (col_shift - j) % 32)
        for r in range(8)
        for j in range(32)
    ]
    return lax.ppermute(value, ("row", "col"), pairs)


def spread(value):
    value = jnp.where(lax.axis_index("row") == 0, value, 0.0)
    for step in (4, 2, 1):
        pairs = [(r, r + step) for r in range(0, 8, 2 * step)]
        value = value + lax.ppermute(value, "row", pairs)
    return value


def on_device(charge, green):
    along_table, back_table, forward, backward = (jnp.asarray(t) for t in tables())
    mirror = reflect(green[SLOTS:], 7, 31)
    mirror_edge = reflect(green[SLOTS:, 0], 7, 32)
    start = reflect(green[0], 8, 31)
    start_edge = reflect(jnp.broadcast_to(green[0, :1], (8, M)), 8, 32)
    zero = spread(jnp.concatenate([green[0], start, start_edge], 0))
    late = (lax.axis_index("row") >= 4).astype(jnp.int32)[None]
    turned = call(
        turn_green, (8, M, LANES), 60, late, green, mirror, mirror_edge, start, start_edge, zero,
        scalars=1,
    )

    along_z = call(z_forward, (8, LANES, LANES), 60, charge.reshape(256, N), along_table)
    by_rows = exchange(along_z, "row").reshape(1024, LANES)
    along_y = call(y_forward, (32, 8, 8, LANES), 60, by_rows, forward)
    by_cols = exchange(along_y.reshape(32, HALF, LANES), "col").reshape(2048, LANES)
    back_x = call(x_both, (2048, LANES), 16, by_cols, turned, forward, backward)
    by_cells = exchange(back_x.reshape(32, HALF, LANES), "col")
    back_y = call(y_backward, (1024, LANES), 16, by_cells.reshape(32, 8, 8, LANES), backward)
    by_parts = exchange(back_y.reshape(8, LANES, LANES), "row")
    back_z = call(z_backward, (256, N), 16, by_parts, back_table)
    return back_z.reshape(8, 32, N)


def solution(mesh):
    in_specs = (P("col", "row", None), P("row", "col", None))
    out_specs = P("col", "row", None)
    return jax.shard_map(
        on_device, mesh=mesh, in_specs=in_specs, out_specs=out_specs, check_vma=False
    )
```

```python
import functools

import jax
import jax.numpy as jnp
import ml_dtypes
import numpy as np
from jax import lax
from jax.experimental import pallas as pl
from jax.experimental.pallas import tpu as pltpu
from jax.sharding import PartitionSpec as P


M = 512
N = 256
LANES = 128
HALF = 64
SLOTS = 32
BF16 = jnp.bfloat16


def split_table(table):
    high = table.astype(ml_dtypes.bfloat16)
    low = (table - high.astype(np.float64)).astype(ml_dtypes.bfloat16)
    return high, low


@functools.cache
def tables():
    freq = np.arange(N)[:, None]
    pair = np.arange(N // 2)[None, :]
    forward = []
    for parity in range(2):
        angle = 2.0 * np.pi * ((freq * (2 * pair + parity)) % M) / M
        forward.append(np.concatenate([np.cos(angle), np.sin(angle)], 1))
    forward = np.stack(forward)
    freq = np.arange(8)[:, None] * HALF + np.arange(SLOTS)[None, :]
    freq[:4, 0] += SLOTS
    angle = 2.0 * np.pi * ((freq[:, :, None] * np.arange(N)) % M) / M
    along_z = np.concatenate([np.cos(angle), -np.sin(angle)], 1).reshape(M, N)
    return tuple(
        np.stack(split_table(t)) for t in (along_z, forward, forward.transpose(0, 2, 1))
    )


def halves(value):
    high = value.astype(BF16)
    low = (value - high.astype(jnp.float32)).astype(BF16)
    return high, low


def mul(left, right, dims=((1,), (0,))):
    dot = functools.partial(
        lax.dot_general, dimension_numbers=(dims, ((), ())), preferred_element_type=jnp.float32
    )
    (lh, ll), (rh, rl) = left, right
    return dot(lh, rh) + (dot(lh, rl) + dot(ll, rh))


def real_lanes(value):
    return lax.broadcasted_iota(jnp.int32, value.shape, 1) % HALF < SLOTS


def forward_rows(data):
    after, before = pltpu.roll(data, LANES - SLOTS, 1), pltpu.roll(data, SLOTS, 1)
    return jnp.concatenate([data, jnp.where(real_lanes(data), after, -before)], 0)


def backward_join(both):
    n = both.shape[0] // 2
    sine = both[n:]
    after, before = pltpu.roll(sine, LANES - SLOTS, 1), pltpu.roll(sine, SLOTS, 1)
    return both[:n] + jnp.where(real_lanes(sine), -after, before)


def trade(first, second):
    low = lax.broadcasted_iota(jnp.int32, first.shape, 1) < HALF
    turned = [pltpu.roll(v, HALF, 1) for v in (first, second)]
    return jnp.where(low, first, turned[1]), jnp.where(low, turned[0], second)


def z_forward(charge, table, out):
    value = halves(charge[...])
    for q in range(4):
        rows = slice(LANES * q, LANES * (q + 1))
        pair = mul(value, (table[0, rows], table[1, rows]), ((1,), (1,)))
        out[2 * q], out[2 * q + 1] = trade(pair[:LANES], pair[LANES:])


def both_parities(table, cols):
    return [
        mul((table[0, p], table[1, p]), halves(jnp.concatenate([forward_rows(c) for c in cols[p]], 1)))
        for p in range(2)
    ]


def y_forward(data, table, out, held):
    for k in range(2):
        cols = [
            [
                jnp.concatenate(
                    [data[pl.ds(128 * s + 32 * (2 * k + i) + p, 16, stride=2), :] for s in range(8)], 0
                )
                for i in range(2)
            ]
            for p in range(2)
        ]
        even, odd = both_parities(table, cols)
        for i in range(2):
            at = slice(LANES * i, LANES * (i + 1))
            for h, value in enumerate((even[:, at] + odd[:, at], even[:, at] - odd[:, at])):
                at_b = N * (2 * i + h)
                held[pl.ds(at_b, N), :] = value
                pair = trade(*(held[pl.ds(at_b + t, LANES, stride=2), :] for t in range(2)))
                for x in range(2):
                    out[16 * h : 16 * (h + 1), 4 * x + 2 * k + i] = pair[x].reshape(16, 8, LANES)


def y_backward(data, backward, out, held):
    for k in range(2):
        low_high = []
        for h in range(2):
            part = []
            for i in range(2):
                pair = trade(
                    *(
                        data[16 * h : 16 * (h + 1), 4 * x + 2 * k + i].reshape(LANES, LANES)
                        for x in range(2)
                    )
                )
                at_b = N * (2 * i + h)
                for t in range(2):
                    held[pl.ds(at_b + t, LANES, stride=2), :] = pair[t]
                part.append(held[pl.ds(at_b, N), :])
            low_high.append(jnp.concatenate(part, 1))
        low, high = low_high
        for p, value in enumerate((low + high, low - high)):
            both = mul((backward[0, p], backward[1, p]), halves(value))
            for i in range(2):
                field = backward_join(both[:, LANES * i : LANES * (i + 1)])
                for s in range(8):
                    rows = pl.ds(128 * s + 32 * (2 * k + i) + p, 16, stride=2)
                    out[rows, :] = field[16 * s : 16 * (s + 1)]


def z_backward(data, table, out):
    total = 0.0
    for q in range(4):
        rows = slice(LANES * q, LANES * (q + 1))
        pair = jnp.concatenate(trade(data[2 * q], data[2 * q + 1]), 0)
        total += mul(halves(pair), (table[0, rows], table[1, rows]))
    out[...] = total * (1.0 / M**3)


def turn_green(up, late, green, middle, mirror, mirror_up, mirror_edge, start, start_edge, zero, out):
    late, own_mirror = late[0] > 0, late[0] > 1
    slot = lax.broadcasted_iota(jnp.int32, (SLOTS, M), 0)
    sign = jnp.where(slot % 2 == 1, 1.0, -1.0)
    share = jnp.where((slot == 0) & own_mirror, 0.5, 1.0)
    row, col = (lax.broadcasted_iota(jnp.int32, (M, M), d) for d in range(2))
    swap = jnp.where((row + col) % M == 0, 1.0, 0.0).astype(BF16)
    row, col = (lax.broadcasted_iota(jnp.int32, (LANES, HALF), d) for d in range(2))
    same = (row // HALF == col // SLOTS) & ((row + col) % SLOTS == 0)
    turn = jnp.where(same, 1.0, 0.0).astype(BF16)
    dot = functools.partial(lax.dot_general, preferred_element_type=jnp.float32)
    nn, nt = (((1,), (0,)), ((), ())), (((1,), (1,)), ((), ()))

    def rows(array, at):
        return jnp.broadcast_to(array[at : at + 1, :], (SLOTS, M))

    for k in range(4):
        owns, others = [], []
        for b in (8 * up + 2 * k, 8 * up + 2 * k + 1):
            at = b - 8 * up
            mid = jnp.broadcast_to(middle[0, at : at + 1, :], (SLOTS, M))
            own = jnp.where((slot == 0) & ~late, mid, green[:, at, :])
            owns.append((own + sign * rows(zero, b)) * share)
            if b == 0:
                other, begin, nil = mirror_edge[...], rows(start_edge, 0), rows(zero, 32)
            else:
                other = mirror[:, 8 - b, :] if b <= 8 else mirror_up[:, 16 - b, :]
                begin, nil = rows(start, 16 - b), rows(zero, 32 - b)
            other = jnp.where((slot == 0) & late, begin, other)
            others.append((other + sign * nil) * share)
        own = jnp.concatenate([owns[0], owns[0], owns[1], owns[1]], 0)
        oh, ol = halves(jnp.concatenate(others, 0))
        oh, ol = halves(dot(turn, oh, nn) + dot(turn, ol, nn))
        out[k] = own.T + (dot(swap, oh, nt) + dot(swap, ol, nt))


def turn_first(late, green, middle, mirror, mirror_edge, start, start_edge, zero, out):
    turn_green(0, late, green, middle, mirror, None, mirror_edge, start, start_edge, zero, out)


def x_both(
    late, green, middle, data, turned, mirror, mirror_up, start, zero, forward, backward, out, turned_up
):
    turn_green(1, late, green, middle, mirror, mirror_up, None, start, None, zero, turned_up)

    def step(own, at, k):
        k = at + 2 * k
        cols = [
            [data[pl.ds(8 * p + k + i, LANES, stride=16), :] for i in range(2)] for p in range(2)
        ]
        even, odd = both_parities(forward, cols)
        low, high = (
            jnp.concatenate([own[k - at + i, N * h : N * (h + 1)] for i in range(2)], 1)
            for h in range(2)
        )
        low, high = (even + odd) * low, (even - odd) * high
        for p, value in enumerate((low + high, low - high)):
            both = mul((backward[0, p], backward[1, p]), halves(value))
            for i in range(2):
                field = backward_join(both[:, LANES * i : LANES * (i + 1)])
                out[pl.ds(8 * p + k + i, LANES, stride=16), :] = field

    for at, own in ((0, turned), (4, turned_up)):
        for k in range(2):
            step(own, at, k)


def call(body, shape, grant, *args, scalars=0, scratch=(), blocks=()):
    vmem, smem = (pl.BlockSpec(memory_space=m) for m in (pltpu.VMEM, pltpu.SMEM))
    return pl.pallas_call(
        body,
        out_shape=jax.ShapeDtypeStruct(shape, jnp.float32),
        grid=(1,) if blocks else (),
        in_specs=[smem] * scalars + [*blocks] + [vmem] * (len(args) - scalars - len(blocks)),
        out_specs=vmem,
        scratch_shapes=[pltpu.VMEM(s, jnp.float32) for s in scratch],
        compiler_params=pltpu.CompilerParams(vmem_limit_bytes=grant * 1024 * 1024),
        cost_estimate=pl.CostEstimate(
            flops=10**9, bytes_accessed=4 * int(np.prod(shape)), transcendentals=0
        ),
    )(*args)


def green_blocks(up):
    return [
        pl.BlockSpec((SLOTS, 8, M), lambda i: (0, up, 0)),
        pl.BlockSpec((1, 8, M), lambda i: (SLOTS, up, 0)),
    ]


def exchange(value, axis):
    return lax.all_to_all(value, axis, split_axis=0, concat_axis=0, tiled=True)


def reflect(value, row_shift, col_shift):
    pairs = [
        (32 * r + j, 32 * ((row_shift - r) % 8) + (col_shift - j) % 32)
        for r in range(8)
        for j in range(32)
    ]
    return lax.ppermute(value, ("row", "col"), pairs)


def spread(value):
    value = jnp.where(lax.axis_index("row") == 0, value, 0.0)
    for step in (4, 2, 1):
        pairs = [(r, r + step) for r in range(0, 8, 2 * step)]
        value = value + lax.ppermute(value, "row", pairs)
    return value


def on_device(charge, green):
    z_table, forward, backward = (jnp.asarray(t) for t in tables())
    moves = {
        "mirror": ("col", [(j, j ^ 29) for j in range(32)]),
        "across": (("row", "col"), [(i, i ^ 226) for i in range(256)]),
    }
    mirrors = []
    for k, order in enumerate((("mirror", "across"), ("across", "mirror"))):
        half = green[SLOTS:, 8 * (1 - k) : 8 * (2 - k)]
        for name in order:
            half = lax.ppermute(half, *moves[name])
        mirrors.append(half)
    mirror_edge = reflect(green[SLOTS:, 0], 7, 32)
    start = reflect(green[0], 8, 31)
    start_edge = reflect(jnp.broadcast_to(green[0, :1], (8, M)), 8, 32)
    zero = spread(jnp.concatenate([green[0], start, start_edge], 0))
    row = lax.axis_index("row")
    late = ((row >= 4).astype(jnp.int32) + (row == 4).astype(jnp.int32))[None]
    turned = call(
        turn_first, (4, M, LANES), 60, late, green, green, mirrors[0], mirror_edge, start, start_edge,
        zero, scalars=1, blocks=green_blocks(0),
    )
    along_z = call(z_forward, (8, LANES, LANES), 60, charge.reshape(256, N), z_table)
    by_rows = exchange(along_z, "row").reshape(1024, LANES)
    along_y = call(y_forward, (32, 8, 8, LANES), 60, by_rows, forward, scratch=[(2 * M, LANES)])
    by_cols = exchange(along_y.reshape(32, HALF, LANES), "col").reshape(2048, LANES)
    back_x = call(
        x_both, (2048, LANES), 60, late, green, green, by_cols, turned, *mirrors, start, zero,
        forward, backward, scalars=1, blocks=green_blocks(1), scratch=[(4, M, LANES)],
    )
    by_cells = exchange(back_x.reshape(32, HALF, LANES), "col")
    back_y = call(
        y_backward, (1024, LANES), 16, by_cells.reshape(32, 8, 8, LANES), backward,
        scratch=[(2 * M, LANES)],
    )
    by_parts = exchange(back_y.reshape(8, LANES, LANES), "row")
    back_z = call(z_backward, (256, N), 16, by_parts, z_table)
    return back_z.reshape(8, 32, N)


def solution(mesh):
    in_specs = (P("col", "row", None), P("row", "col", None))
    out_specs = P("col", "row", None)
    return jax.shard_map(
        on_device, mesh=mesh, in_specs=in_specs, out_specs=out_specs, check_vma=False
    )
```

```python
import functools

import jax
import jax.numpy as jnp
import ml_dtypes
import numpy as np
from jax import lax
from jax.experimental import pallas as pl
from jax.experimental.pallas import tpu as pltpu
from jax.sharding import PartitionSpec as P


M = 512
N = 256
LANES = 128
HALF = 64
SLOTS = 32
BF16 = jnp.bfloat16


def split_table(table):
    high = table.astype(ml_dtypes.bfloat16)
    low = (table - high.astype(np.float64)).astype(ml_dtypes.bfloat16)
    return high, low


@functools.cache
def tables():
    freq = np.arange(N)[:, None]
    pair = np.arange(N // 2)[None, :]
    forward = []
    for parity in range(2):
        angle = 2.0 * np.pi * ((freq * (2 * pair + parity)) % M) / M
        forward.append(np.concatenate([np.cos(angle), np.sin(angle)], 1))
    forward = np.stack(forward)
    freq = np.arange(8)[:, None] * HALF + np.arange(SLOTS)[None, :]
    freq[:4, 0] += SLOTS
    angle = 2.0 * np.pi * ((freq[:, :, None] * np.arange(N)) % M) / M
    along_z = np.concatenate([np.cos(angle), -np.sin(angle)], 1).reshape(M, N)
    return tuple(
        np.stack(split_table(t)) for t in (along_z, forward, forward.transpose(0, 2, 1))
    )


def halves(value):
    high = value.astype(BF16)
    low = (value - high.astype(jnp.float32)).astype(BF16)
    return high, low


def mul(left, right, dims=((1,), (0,))):
    dot = functools.partial(
        lax.dot_general, dimension_numbers=(dims, ((), ())), preferred_element_type=jnp.float32
    )
    (lh, ll), (rh, rl) = left, right
    return dot(lh, rh) + (dot(lh, rl) + dot(ll, rh))


def real_lanes(value):
    return lax.broadcasted_iota(jnp.int32, value.shape, 1) % HALF < SLOTS


def forward_rows(data):
    after, before = pltpu.roll(data, LANES - SLOTS, 1), pltpu.roll(data, SLOTS, 1)
    return jnp.concatenate([data, jnp.where(real_lanes(data), after, -before)], 0)


def backward_join(both):
    n = both.shape[0] // 2
    sine = both[n:]
    after, before = pltpu.roll(sine, LANES - SLOTS, 1), pltpu.roll(sine, SLOTS, 1)
    return both[:n] + jnp.where(real_lanes(sine), -after, before)


def trade(first, second):
    low = lax.broadcasted_iota(jnp.int32, first.shape, 1) < HALF
    turned = [pltpu.roll(v, HALF, 1) for v in (first, second)]
    return jnp.where(low, first, turned[1]), jnp.where(low, turned[0], second)


def z_forward(charge, table, out):
    value = halves(charge[...])
    for q in range(4):
        rows = slice(LANES * q, LANES * (q + 1))
        pair = mul(value, (table[0, rows], table[1, rows]), ((1,), (1,)))
        out[2 * q], out[2 * q + 1] = trade(pair[:LANES], pair[LANES:])


def both_parities(table, cols):
    return [
        mul((table[0, p], table[1, p]), halves(jnp.concatenate([forward_rows(c) for c in cols[p]], 1)))
        for p in range(2)
    ]


def y_forward(data, table, out, held):
    for k in range(2):
        cols = [
            [
                jnp.concatenate(
                    [data[pl.ds(128 * s + 32 * (2 * k + i) + p, 16, stride=2), :] for s in range(8)], 0
                )
                for i in range(2)
            ]
            for p in range(2)
        ]
        even, odd = both_parities(table, cols)
        for i in range(2):
            at = slice(LANES * i, LANES * (i + 1))
            for h, value in enumerate((even[:, at] + odd[:, at], even[:, at] - odd[:, at])):
                at_b = N * (2 * i + h)
                held[pl.ds(at_b, N), :] = value
                pair = trade(*(held[pl.ds(at_b + t, LANES, stride=2), :] for t in range(2)))
                for x in range(2):
                    out[16 * h : 16 * (h + 1), 4 * x + 2 * k + i] = pair[x].reshape(16, 8, LANES)


def y_backward(data, backward, out, held):
    for k in range(2):
        low_high = []
        for h in range(2):
            part = []
            for i in range(2):
                pair = trade(
                    *(
                        data[16 * h : 16 * (h + 1), 4 * x + 2 * k + i].reshape(LANES, LANES)
                        for x in range(2)
                    )
                )
                at_b = N * (2 * i + h)
                for t in range(2):
                    held[pl.ds(at_b + t, LANES, stride=2), :] = pair[t]
                part.append(held[pl.ds(at_b, N), :])
            low_high.append(jnp.concatenate(part, 1))
        low, high = low_high
        for p, value in enumerate((low + high, low - high)):
            both = mul((backward[0, p], backward[1, p]), halves(value))
            for i in range(2):
                field = backward_join(both[:, LANES * i : LANES * (i + 1)])
                for s in range(8):
                    rows = pl.ds(128 * s + 32 * (2 * k + i) + p, 16, stride=2)
                    out[rows, :] = field[16 * s : 16 * (s + 1)]


def z_backward(data, table, out):
    total = 0.0
    for q in range(4):
        rows = slice(LANES * q, LANES * (q + 1))
        pair = jnp.concatenate(trade(data[2 * q], data[2 * q + 1]), 0)
        total += mul(halves(pair), (table[0, rows], table[1, rows]))
    out[...] = total * (1.0 / M**3)


def turn_green(up, late, green, middle, mirror, mirror_up, mirror_edge, start, start_edge, zero, out):
    late, own_mirror = late[0] > 0, late[0] > 1
    slot = lax.broadcasted_iota(jnp.int32, (SLOTS, M), 0)
    sign = jnp.where(slot % 2 == 1, 1.0, -1.0)
    share = jnp.where((slot == 0) & own_mirror, 0.5, 1.0)
    row, col = (lax.broadcasted_iota(jnp.int32, (M, M), d) for d in range(2))
    swap = jnp.where((row + col) % M == 0, 1.0, 0.0).astype(BF16)
    row, col = (lax.broadcasted_iota(jnp.int32, (LANES, HALF), d) for d in range(2))
    same = (row // HALF == col // SLOTS) & ((row + col) % SLOTS == 0)
    turn = jnp.where(same, 1.0, 0.0).astype(BF16)
    dot = functools.partial(lax.dot_general, preferred_element_type=jnp.float32)
    nn, nt = (((1,), (0,)), ((), ())), (((1,), (1,)), ((), ()))

    def rows(array, at):
        return jnp.broadcast_to(array[at : at + 1, :], (SLOTS, M))

    for k in range(4):
        owns, others = [], []
        for b in (8 * up + 2 * k, 8 * up + 2 * k + 1):
            at = b - 8 * up
            mid = jnp.broadcast_to(middle[0, at : at + 1, :], (SLOTS, M))
            own = jnp.where((slot == 0) & ~late, mid, green[:, at, :])
            owns.append((own + sign * rows(zero, b)) * share)
            if b == 0:
                other, begin, nil = mirror_edge[...], rows(start_edge, 0), rows(zero, 32)
            else:
                other = mirror[:, 8 - b, :] if b <= 8 else mirror_up[:, 16 - b, :]
                begin, nil = rows(start, 16 - b), rows(zero, 32 - b)
            other = jnp.where((slot == 0) & late, begin, other)
            others.append((other + sign * nil) * share)
        own = jnp.concatenate([owns[0], owns[0], owns[1], owns[1]], 0)
        oh, ol = halves(jnp.concatenate(others, 0))
        oh, ol = halves(dot(turn, oh, nn) + dot(turn, ol, nn))
        out[k] = own.T + (dot(swap, oh, nt) + dot(swap, ol, nt))


def turn_first(late, green, middle, mirror, mirror_edge, start, start_edge, zero, out):
    turn_green(0, late, green, middle, mirror, None, mirror_edge, start, start_edge, zero, out)


def turn_second(late, green, middle, mirror, mirror_up, start, zero, out):
    turn_green(1, late, green, middle, mirror, mirror_up, None, start, None, zero, out)


def x_both(data, turned, turned_up, forward, backward, out):
    def step(own, at, k):
        k = at + 2 * k
        cols = [
            [data[pl.ds(8 * p + k + i, LANES, stride=16), :] for i in range(2)] for p in range(2)
        ]
        even, odd = both_parities(forward, cols)
        low, high = (
            jnp.concatenate([own[k - at + i, N * h : N * (h + 1)] for i in range(2)], 1)
            for h in range(2)
        )
        low, high = (even + odd) * low, (even - odd) * high
        for p, value in enumerate((low + high, low - high)):
            both = mul((backward[0, p], backward[1, p]), halves(value))
            for i in range(2):
                field = backward_join(both[:, LANES * i : LANES * (i + 1)])
                out[pl.ds(8 * p + k + i, LANES, stride=16), :] = field

    for at, own in ((0, turned), (4, turned_up)):
        for k in range(2):
            step(own, at, k)


def call(body, shape, grant, *args, scalars=0, scratch=(), blocks=()):
    vmem, smem = (pl.BlockSpec(memory_space=m) for m in (pltpu.VMEM, pltpu.SMEM))
    return pl.pallas_call(
        body,
        out_shape=jax.ShapeDtypeStruct(shape, jnp.float32),
        grid=(1,) if blocks else (),
        in_specs=[smem] * scalars + [*blocks] + [vmem] * (len(args) - scalars - len(blocks)),
        out_specs=vmem,
        scratch_shapes=scratch,
        compiler_params=pltpu.CompilerParams(vmem_limit_bytes=grant * 1024 * 1024),
        cost_estimate=pl.CostEstimate(
            flops=10**9, bytes_accessed=4 * int(np.prod(shape)), transcendentals=0
        ),
    )(*args)


def green_blocks(up):
    return [
        pl.BlockSpec((SLOTS, 8, M), lambda i: (0, up, 0)),
        pl.BlockSpec((1, 8, M), lambda i: (SLOTS, up, 0)),
    ]


def exchange(value, axis):
    return lax.all_to_all(value, axis, split_axis=0, concat_axis=0, tiled=True)


def reflect(value, row_shift, col_shift):
    pairs = [
        (32 * r + j, 32 * ((row_shift - r) % 8) + (col_shift - j) % 32)
        for r in range(8)
        for j in range(32)
    ]
    return lax.ppermute(value, ("row", "col"), pairs)


def spread(value):
    value = jnp.where(lax.axis_index("row") == 0, value, 0.0)
    for step in (4, 2, 1):
        pairs = [(r, r + step) for r in range(0, 8, 2 * step)]
        value = value + lax.ppermute(value, "row", pairs)
    return value


def on_device(charge, green):
    z_table, forward, backward = (jnp.asarray(t) for t in tables())
    along_z = call(z_forward, (8, LANES, LANES), 60, charge.reshape(256, N), z_table)
    later, along_z = lax.optimization_barrier((green, along_z))
    moves = {
        "mirror": ("col", [(j, j ^ 29) for j in range(32)]),
        "across": (("row", "col"), [(i, i ^ 226) for i in range(256)]),
    }
    mirrors = []
    for k, order in enumerate((("mirror", "across"), ("across", "mirror"))):
        half = (green, later)[k][SLOTS:, 8 * (1 - k) : 8 * (2 - k)]
        for name in order:
            half = lax.ppermute(half, *moves[name])
        mirrors.append(half)
    mirror_edge = reflect(green[SLOTS:, 0], 7, 32)
    start = reflect(green[0], 8, 31)
    start_edge = reflect(jnp.broadcast_to(green[0, :1], (8, M)), 8, 32)
    zero = spread(jnp.concatenate([green[0], start, start_edge], 0))
    row = lax.axis_index("row")
    late = ((row >= 4).astype(jnp.int32) + (row == 4).astype(jnp.int32))[None]
    turned = call(
        turn_first, (4, M, LANES), 60, late, green, green, mirrors[0], mirror_edge, start, start_edge,
        zero, scalars=1, blocks=green_blocks(0),
    )
    turned_up = call(
        turn_second, (4, M, LANES), 60, late, green, green, *mirrors, start, zero,
        scalars=1, blocks=green_blocks(1),
    )
    by_rows = exchange(along_z, "row").reshape(1024, LANES)
    along_y = call(y_forward, (32, 8, 8, LANES), 16, by_rows, forward, scratch=[pltpu.VMEM((2 * M, LANES), jnp.float32)])
    by_cols = exchange(along_y.reshape(32, HALF, LANES), "col").reshape(2048, LANES)
    back_x = call(x_both, (2048, LANES), 24, by_cols, turned, turned_up, forward, backward)
    by_cells = exchange(back_x.reshape(32, HALF, LANES), "col")
    back_y = call(
        y_backward, (1024, LANES), 16, by_cells.reshape(32, 8, 8, LANES), backward,
        scratch=[pltpu.VMEM((2 * M, LANES), jnp.float32)],
    )
    by_parts = exchange(back_y.reshape(8, LANES, LANES), "row")
    back_z = call(z_backward, (256, N), 16, by_parts, z_table)
    return back_z.reshape(8, 32, N)


def solution(mesh):
    in_specs = (P("col", "row", None), P("row", "col", None))
    out_specs = P("col", "row", None)
    return jax.shard_map(
        on_device, mesh=mesh, in_specs=in_specs, out_specs=out_specs, check_vma=False
    )
```

```python
import functools

import jax
import jax.numpy as jnp
import ml_dtypes
import numpy as np
from jax import lax
from jax.experimental import pallas as pl
from jax.experimental.pallas import tpu as pltpu
from jax.sharding import PartitionSpec as P


M = 512
N = 256
LANES = 128
HALF = 64
SLOTS = 32
BF16 = jnp.bfloat16


def split_table(table):
    high = table.astype(ml_dtypes.bfloat16)
    low = (table - high.astype(np.float64)).astype(ml_dtypes.bfloat16)
    return high, low


@functools.cache
def tables():
    freq = np.arange(N)[:, None]
    pair = np.arange(N // 2)[None, :]
    forward = []
    for parity in range(2):
        angle = 2.0 * np.pi * ((freq * (2 * pair + parity)) % M) / M
        forward.append(np.concatenate([np.cos(angle), np.sin(angle)], 1))
    forward = np.stack(forward)
    freq = np.arange(8)[:, None] * HALF + np.arange(SLOTS)[None, :]
    freq[:4, 0] += SLOTS
    angle = 2.0 * np.pi * ((freq[:, :, None] * np.arange(N)) % M) / M
    along_z = np.concatenate([np.cos(angle), -np.sin(angle)], 1).reshape(M, N)
    return tuple(
        np.stack(split_table(t)) for t in (along_z, forward, forward.transpose(0, 2, 1))
    )


def halves(value):
    high = value.astype(BF16)
    low = (value - high.astype(jnp.float32)).astype(BF16)
    return high, low


def mul(left, right, dims=((1,), (0,))):
    dot = functools.partial(
        lax.dot_general, dimension_numbers=(dims, ((), ())), preferred_element_type=jnp.float32
    )
    (lh, ll), (rh, rl) = left, right
    return dot(lh, rh) + (dot(lh, rl) + dot(ll, rh))


def real_lanes(value):
    return lax.broadcasted_iota(jnp.int32, value.shape, 1) % HALF < SLOTS


def forward_rows(data):
    after, before = pltpu.roll(data, LANES - SLOTS, 1), pltpu.roll(data, SLOTS, 1)
    return jnp.concatenate([data, jnp.where(real_lanes(data), after, -before)], 0)


def backward_join(both):
    n = both.shape[0] // 2
    sine = both[n:]
    after, before = pltpu.roll(sine, LANES - SLOTS, 1), pltpu.roll(sine, SLOTS, 1)
    return both[:n] + jnp.where(real_lanes(sine), -after, before)


def trade(first, second):
    low = lax.broadcasted_iota(jnp.int32, first.shape, 1) < HALF
    turned = [pltpu.roll(v, HALF, 1) for v in (first, second)]
    return jnp.where(low, first, turned[1]), jnp.where(low, turned[0], second)


def z_forward(charge, table, out):
    value = halves(charge[...])
    for q in range(4):
        rows = slice(LANES * q, LANES * (q + 1))
        pair = mul(value, (table[0, rows], table[1, rows]), ((1,), (1,)))
        out[2 * q], out[2 * q + 1] = trade(pair[:LANES], pair[LANES:])


def both_parities(table, cols):
    return [
        mul((table[0, p], table[1, p]), halves(jnp.concatenate([forward_rows(c) for c in cols[p]], 1)))
        for p in range(2)
    ]


def y_forward(data, table, out, held):
    for k in range(2):
        cols = [
            [
                jnp.concatenate(
                    [data[pl.ds(128 * s + 32 * (2 * k + i) + p, 16, stride=2), :] for s in range(8)], 0
                )
                for i in range(2)
            ]
            for p in range(2)
        ]
        even, odd = both_parities(table, cols)
        for i in range(2):
            at = slice(LANES * i, LANES * (i + 1))
            for h, value in enumerate((even[:, at] + odd[:, at], even[:, at] - odd[:, at])):
                at_b = N * (2 * i + h)
                held[pl.ds(at_b, N), :] = value
                pair = trade(*(held[pl.ds(at_b + t, LANES, stride=2), :] for t in range(2)))
                for x in range(2):
                    out[16 * h : 16 * (h + 1), 4 * x + 2 * k + i] = pair[x].reshape(16, 8, LANES)


def y_backward(data, backward, out, held):
    for k in range(2):
        low_high = []
        for h in range(2):
            part = []
            for i in range(2):
                pair = trade(
                    *(
                        data[16 * h : 16 * (h + 1), 4 * x + 2 * k + i].reshape(LANES, LANES)
                        for x in range(2)
                    )
                )
                at_b = N * (2 * i + h)
                for t in range(2):
                    held[pl.ds(at_b + t, LANES, stride=2), :] = pair[t]
                part.append(held[pl.ds(at_b, N), :])
            low_high.append(jnp.concatenate(part, 1))
        low, high = low_high
        for p, value in enumerate((low + high, low - high)):
            both = mul((backward[0, p], backward[1, p]), halves(value))
            for i in range(2):
                field = backward_join(both[:, LANES * i : LANES * (i + 1)])
                for s in range(8):
                    rows = pl.ds(128 * s + 32 * (2 * k + i) + p, 16, stride=2)
                    out[rows, :] = field[16 * s : 16 * (s + 1)]


def z_backward(data, table, out):
    total = 0.0
    for q in range(4):
        rows = slice(LANES * q, LANES * (q + 1))
        pair = jnp.concatenate(trade(data[2 * q], data[2 * q + 1]), 0)
        total += mul(halves(pair), (table[0, rows], table[1, rows]))
    out[...] = total * (1.0 / M**3)


def turn_green(lows, base, late, green, middle, low, high, mirror_edge, start, start_edge, zero, out):
    late, own_mirror = late[0] > 0, late[0] > 1
    slot = lax.broadcasted_iota(jnp.int32, (SLOTS, M), 0)
    sign = jnp.where(slot % 2 == 1, 1.0, -1.0)
    share = jnp.where((slot == 0) & own_mirror, 0.5, 1.0)
    row, col = (lax.broadcasted_iota(jnp.int32, (M, M), d) for d in range(2))
    swap = jnp.where((row + col) % M == 0, 1.0, 0.0).astype(BF16)
    row, col = (lax.broadcasted_iota(jnp.int32, (LANES, HALF), d) for d in range(2))
    same = (row // HALF == col // SLOTS) & ((row + col) % SLOTS == 0)
    turn = jnp.where(same, 1.0, 0.0).astype(BF16)
    dot = functools.partial(lax.dot_general, preferred_element_type=jnp.float32)
    nn, nt = (((1,), (0,)), ((), ())), (((1,), (1,)), ((), ()))

    def rows(array, at):
        return jnp.broadcast_to(array[at : at + 1, :], (SLOTS, M))

    parts = []
    for k, b_low in enumerate(lows):
        owns, others = [], []
        for b in (2 * b_low, 2 * b_low + 1):
            at = b - base
            mid = jnp.broadcast_to(middle[0, at : at + 1, :], (SLOTS, M))
            own = jnp.where((slot == 0) & ~late, mid, green[:, at, :])
            owns.append((own + sign * rows(zero, b)) * share)
            if b == 0:
                other, begin, nil = mirror_edge[...], rows(start_edge, 0), rows(zero, 32)
            else:
                other = high[:, 8 - b, :] if b <= 8 else low[:, 16 - b, :]
                begin, nil = rows(start, 16 - b), rows(zero, 32 - b)
            other = jnp.where((slot == 0) & late, begin, other)
            others.append((other + sign * nil) * share)
        own = jnp.concatenate([owns[0], owns[0], owns[1], owns[1]], 0)
        oh, ol = halves(jnp.concatenate(others, 0))
        parts.append(halves(dot(turn, oh, nn) + dot(turn, ol, nn)))
        out[k] = own.T
    oh, ol = (jnp.concatenate([p[i] for p in parts], 0) for i in range(2))
    both = dot(swap, oh, nt) + dot(swap, ol, nt)
    for k in range(len(lows)):
        out[k] += both[:, LANES * k : LANES * (k + 1)]


def turn_first(late, green, middle, low, start, zero, out):
    turn_green(range(5, 8), 8, late, green, middle, low, None, None, start, None, zero, out)


def turn_second(late, green, middle, low, high, mirror_edge, start, start_edge, zero, out):
    turn_green(
        range(5), 0, late, green, middle, low, high, mirror_edge, start, start_edge, zero, out
    )


def x_both(data, turned_up, turned, forward, backward, out):
    def green(b_low, h):
        own, at = (turned, b_low) if b_low < 5 else (turned_up, b_low - 5)
        return own[at, N * h : N * (h + 1)]

    for k in range(0, 8, 2):
        cols = [
            [data[pl.ds(8 * p + k + i, LANES, stride=16), :] for i in range(2)] for p in range(2)
        ]
        even, odd = both_parities(forward, cols)
        low, high = (
            jnp.concatenate([green(k + i, h) for i in range(2)], 1)
            for h in range(2)
        )
        low, high = (even + odd) * low, (even - odd) * high
        for p, value in enumerate((low + high, low - high)):
            both = mul((backward[0, p], backward[1, p]), halves(value))
            for i in range(2):
                field = backward_join(both[:, LANES * i : LANES * (i + 1)])
                out[pl.ds(8 * p + k + i, LANES, stride=16), :] = field


def call(body, shape, grant, *args, scalars=0, scratch=(), blocks=()):
    vmem, smem = (pl.BlockSpec(memory_space=m) for m in (pltpu.VMEM, pltpu.SMEM))
    return pl.pallas_call(
        body,
        out_shape=jax.ShapeDtypeStruct(shape, jnp.float32),
        grid=(1,) if blocks else (),
        in_specs=[smem] * scalars + [*blocks] + [vmem] * (len(args) - scalars - len(blocks)),
        out_specs=vmem,
        scratch_shapes=scratch,
        compiler_params=pltpu.CompilerParams(vmem_limit_bytes=grant * 1024 * 1024),
        cost_estimate=pl.CostEstimate(
            flops=10**9, bytes_accessed=4 * int(np.prod(shape)), transcendentals=0
        ),
    )(*args)


def green_blocks(length, at):
    return [
        pl.BlockSpec((SLOTS, length, M), lambda i: (0, at, 0)),
        pl.BlockSpec((1, length, M), lambda i: (SLOTS, at, 0)),
    ]


def exchange(value, axis):
    return lax.all_to_all(value, axis, split_axis=0, concat_axis=0, tiled=True)


def reflect(value, row_shift, col_shift):
    pairs = [
        (32 * r + j, 32 * ((row_shift - r) % 8) + (col_shift - j) % 32)
        for r in range(8)
        for j in range(32)
    ]
    return lax.ppermute(value, ("row", "col"), pairs)


def spread(value):
    value = jnp.where(lax.axis_index("row") == 0, value, 0.0)
    for step in (4, 2, 1):
        pairs = [(r, r + step) for r in range(0, 8, 2 * step)]
        value = value + lax.ppermute(value, "row", pairs)
    return value


def on_device(charge, green):
    z_table, forward, backward = (jnp.asarray(t) for t in tables())
    along_z = call(z_forward, (8, LANES, LANES), 60, charge.reshape(256, N), z_table)
    later, along_z = lax.optimization_barrier((green, along_z))
    moves = {
        "mirror": ("col", [(j, j ^ 29) for j in range(32)]),
        "across": (("row", "col"), [(i, i ^ 226) for i in range(256)]),
    }
    mirrors = []
    for k, order in enumerate((("mirror", "across"), ("across", "mirror"))):
        half = (green, later)[k][SLOTS:, 8 * k : 8 * (k + 1)]
        for name in order:
            half = lax.ppermute(half, *moves[name])
        mirrors.append(half)
    mirror_edge = reflect(green[SLOTS:, 0], 7, 32)
    start = reflect(green[0], 8, 31)
    start_edge = reflect(jnp.broadcast_to(green[0, :1], (8, M)), 8, 32)
    zero = spread(jnp.concatenate([green[0], start, start_edge], 0))
    row = lax.axis_index("row")
    late = ((row >= 4).astype(jnp.int32) + (row == 4).astype(jnp.int32))[None]
    turned_up = call(
        turn_first, (3, M, LANES), 60, late, green, green, mirrors[0], start, zero,
        scalars=1, blocks=green_blocks(8, 1),
    )
    turned = call(
        turn_second, (5, M, LANES), 60, late, green, green, *mirrors, mirror_edge, start,
        start_edge, zero, scalars=1, blocks=green_blocks(16, 0),
    )
    by_rows = exchange(along_z, "row").reshape(1024, LANES)
    along_y = call(y_forward, (32, 8, 8, LANES), 16, by_rows, forward, scratch=[pltpu.VMEM((2 * M, LANES), jnp.float32)])
    by_cols = exchange(along_y.reshape(32, HALF, LANES), "col").reshape(2048, LANES)
    back_x = call(x_both, (2048, LANES), 24, by_cols, turned_up, turned, forward, backward)
    by_cells = exchange(back_x.reshape(32, HALF, LANES), "col")
    back_y = call(
        y_backward, (1024, LANES), 16, by_cells.reshape(32, 8, 8, LANES), backward,
        scratch=[pltpu.VMEM((2 * M, LANES), jnp.float32)],
    )
    by_parts = exchange(back_y.reshape(8, LANES, LANES), "row")
    back_z = call(z_backward, (256, N), 16, by_parts, z_table)
    return back_z.reshape(8, 32, N)


def solution(mesh):
    in_specs = (P("col", "row", None), P("row", "col", None))
    out_specs = P("col", "row", None)
    return jax.shard_map(
        on_device, mesh=mesh, in_specs=in_specs, out_specs=out_specs, check_vma=False
    )
```

```python
import functools

import jax
import jax.numpy as jnp
import ml_dtypes
import numpy as np
from jax import lax
from jax.experimental import pallas as pl
from jax.experimental.pallas import tpu as pltpu
from jax.sharding import PartitionSpec as P


M = 512
N = 256
LANES = 128
HALF = 64
SLOTS = 32
BF16 = jnp.bfloat16


def split_table(table):
    high = table.astype(ml_dtypes.bfloat16)
    low = (table - high.astype(np.float64)).astype(ml_dtypes.bfloat16)
    return high, low


@functools.cache
def tables():
    freq = np.arange(N)[:, None]
    pair = np.arange(N // 2)[None, :]
    forward = []
    for parity in range(2):
        angle = 2.0 * np.pi * ((freq * (2 * pair + parity)) % M) / M
        forward.append(np.concatenate([np.cos(angle), np.sin(angle)], 1))
    forward = np.stack(forward)
    freq = np.arange(8)[:, None] * HALF + np.arange(SLOTS)[None, :]
    freq[:4, 0] += SLOTS
    angle = 2.0 * np.pi * ((freq[:, :, None] * np.arange(N)) % M) / M
    along_z = np.concatenate([np.cos(angle), -np.sin(angle)], 1).reshape(M, N)
    return tuple(
        np.stack(split_table(t)) for t in (along_z, forward, forward.transpose(0, 2, 1))
    )


def halves(value):
    high = value.astype(BF16)
    low = (value - high.astype(jnp.float32)).astype(BF16)
    return high, low


def mul(left, right, dims=((1,), (0,))):
    dot = functools.partial(
        lax.dot_general, dimension_numbers=(dims, ((), ())), preferred_element_type=jnp.float32
    )
    (lh, ll), (rh, rl) = left, right
    return dot(lh, rh) + (dot(lh, rl) + dot(ll, rh))


def real_lanes(value):
    return lax.broadcasted_iota(jnp.int32, value.shape, 1) % HALF < SLOTS


def forward_rows(data):
    after, before = pltpu.roll(data, LANES - SLOTS, 1), pltpu.roll(data, SLOTS, 1)
    return jnp.concatenate([data, jnp.where(real_lanes(data), after, -before)], 0)


def backward_join(both):
    n = both.shape[0] // 2
    sine = both[n:]
    after, before = pltpu.roll(sine, LANES - SLOTS, 1), pltpu.roll(sine, SLOTS, 1)
    return both[:n] + jnp.where(real_lanes(sine), -after, before)


def trade(first, second):
    low = lax.broadcasted_iota(jnp.int32, first.shape, 1) < HALF
    turned = [pltpu.roll(v, HALF, 1) for v in (first, second)]
    return jnp.where(low, first, turned[1]), jnp.where(low, turned[0], second)


def z_forward(charge, table, out):
    value = halves(charge[...])
    for q in range(4):
        rows = slice(LANES * q, LANES * (q + 1))
        pair = mul(value, (table[0, rows], table[1, rows]), ((1,), (1,)))
        out[2 * q], out[2 * q + 1] = trade(pair[:LANES], pair[LANES:])


def both_parities(table, cols):
    return [
        mul((table[0, p], table[1, p]), halves(jnp.concatenate([forward_rows(c) for c in cols[p]], 1)))
        for p in range(2)
    ]


def y_forward(data, table, out, held):
    for k in range(2):
        cols = [
            [
                jnp.concatenate(
                    [data[pl.ds(128 * s + 32 * (2 * k + i) + p, 16, stride=2), :] for s in range(8)], 0
                )
                for i in range(2)
            ]
            for p in range(2)
        ]
        even, odd = both_parities(table, cols)
        for i in range(2):
            at = slice(LANES * i, LANES * (i + 1))
            for h, value in enumerate((even[:, at] + odd[:, at], even[:, at] - odd[:, at])):
                at_b = N * (2 * i + h)
                held[pl.ds(at_b, N), :] = value
                pair = trade(*(held[pl.ds(at_b + t, LANES, stride=2), :] for t in range(2)))
                for x in range(2):
                    out[16 * h : 16 * (h + 1), 4 * x + 2 * k + i] = pair[x].reshape(16, 8, LANES)


def y_backward(data, backward, out, held):
    for k in range(2):
        low_high = []
        for h in range(2):
            part = []
            for i in range(2):
                pair = trade(
                    *(
                        data[16 * h : 16 * (h + 1), 4 * x + 2 * k + i].reshape(LANES, LANES)
                        for x in range(2)
                    )
                )
                at_b = N * (2 * i + h)
                for t in range(2):
                    held[pl.ds(at_b + t, LANES, stride=2), :] = pair[t]
                part.append(held[pl.ds(at_b, N), :])
            low_high.append(jnp.concatenate(part, 1))
        low, high = low_high
        for p, value in enumerate((low + high, low - high)):
            both = mul((backward[0, p], backward[1, p]), halves(value))
            for i in range(2):
                field = backward_join(both[:, LANES * i : LANES * (i + 1)])
                for s in range(8):
                    rows = pl.ds(128 * s + 32 * (2 * k + i) + p, 16, stride=2)
                    out[rows, :] = field[16 * s : 16 * (s + 1)]


def z_backward(data, table, out):
    total = 0.0
    for q in range(4):
        rows = slice(LANES * q, LANES * (q + 1))
        pair = jnp.concatenate(trade(data[2 * q], data[2 * q + 1]), 0)
        total += mul(halves(pair), (table[0, rows], table[1, rows]))
    out[...] = total * (1.0 / M**3)


def turn_green(lows, base, late, green, middle, low, high, mirror_edge, start, start_edge, zero, out):
    late, own_mirror = late[0] > 0, late[0] > 1
    slot = lax.broadcasted_iota(jnp.int32, (SLOTS, M), 0)
    sign = jnp.where(slot % 2 == 1, 1.0, -1.0)
    share = jnp.where((slot == 0) & own_mirror, 0.5, 1.0)
    row, col = (lax.broadcasted_iota(jnp.int32, (M, M), d) for d in range(2))
    swap = jnp.where((row + col) % M == 0, 1.0, 0.0).astype(BF16)
    row, col = (lax.broadcasted_iota(jnp.int32, (LANES, HALF), d) for d in range(2))
    same = (row // HALF == col // SLOTS) & ((row + col) % SLOTS == 0)
    turn = jnp.where(same, 1.0, 0.0).astype(BF16)
    dot = functools.partial(lax.dot_general, preferred_element_type=jnp.float32)
    nn, nt = (((1,), (0,)), ((), ())), (((1,), (1,)), ((), ()))

    def rows(array, at):
        return jnp.broadcast_to(array[at : at + 1, :], (SLOTS, M))

    parts = []
    for k, b_low in enumerate(lows):
        owns, others = [], []
        for b in (2 * b_low, 2 * b_low + 1):
            at = b - base
            mid = jnp.broadcast_to(middle[0, at : at + 1, :], (SLOTS, M))
            own = jnp.where((slot == 0) & ~late, mid, green[:, at, :])
            owns.append((own + sign * rows(zero, b)) * share)
            if b == 0:
                other, begin, nil = mirror_edge[...], rows(start_edge, 0), rows(zero, 32)
            else:
                other = high[:, 8 - b, :] if b <= 8 else low[:, 16 - b, :]
                begin, nil = rows(start, 16 - b), rows(zero, 32 - b)
            other = jnp.where((slot == 0) & late, begin, other)
            others.append((other + sign * nil) * share)
        own = jnp.concatenate([owns[0], owns[0], owns[1], owns[1]], 0)
        oh, ol = halves(jnp.concatenate(others, 0))
        parts.append(halves(dot(turn, oh, nn) + dot(turn, ol, nn)))
        out[k] = own.T
    oh, ol = (jnp.concatenate([p[i] for p in parts], 0) for i in range(2))
    both = dot(swap, oh, nt) + dot(swap, ol, nt)
    for k in range(len(lows)):
        out[k] += both[:, LANES * k : LANES * (k + 1)]


def turn_first(late, green, middle, low, start, zero, out):
    turn_green(range(5, 8), 8, late, green, middle, low, None, None, start, None, zero, out)


def turn_second(late, green, middle, low, high, mirror_edge, start, start_edge, zero, out):
    turn_green(
        range(5), 0, late, green, middle, low, high, mirror_edge, start, start_edge, zero, out
    )


def x_both(data, turned_up, turned, forward, backward, out):
    def green(b_low, h):
        own, at = (turned, b_low) if b_low < 5 else (turned_up, b_low - 5)
        return own[at, N * h : N * (h + 1)]

    for k in range(0, 8, 2):
        cols = [
            [data[pl.ds(8 * p + k + i, LANES, stride=16), :] for i in range(2)] for p in range(2)
        ]
        even, odd = both_parities(forward, cols)
        low, high = (
            jnp.concatenate([green(k + i, h) for i in range(2)], 1)
            for h in range(2)
        )
        low, high = (even + odd) * low, (even - odd) * high
        for p, value in enumerate((low + high, low - high)):
            both = mul((backward[0, p], backward[1, p]), halves(value))
            for i in range(2):
                field = backward_join(both[:, LANES * i : LANES * (i + 1)])
                out[pl.ds(8 * p + k + i, LANES, stride=16), :] = field


def call(body, shape, grant, *args, scalars=0, scratch=(), blocks=()):
    vmem, smem = (pl.BlockSpec(memory_space=m) for m in (pltpu.VMEM, pltpu.SMEM))
    return pl.pallas_call(
        body,
        out_shape=jax.ShapeDtypeStruct(shape, jnp.float32),
        grid=(1,) if blocks else (),
        in_specs=[smem] * scalars + [*blocks] + [vmem] * (len(args) - scalars - len(blocks)),
        out_specs=vmem,
        scratch_shapes=scratch,
        compiler_params=pltpu.CompilerParams(vmem_limit_bytes=grant * 1024 * 1024),
        cost_estimate=pl.CostEstimate(
            flops=10**9, bytes_accessed=4 * int(np.prod(shape)), transcendentals=0
        ),
    )(*args)


def green_blocks(length, at):
    return [
        pl.BlockSpec((SLOTS, length, M), lambda i: (0, at, 0)),
        pl.BlockSpec((1, length, M), lambda i: (SLOTS, at, 0)),
    ]


def pack_edges(upper, plane, edge, start, start_edge):
    edge[...] = upper[:, 0, :]
    start[...] = plane[0]
    start_edge[...] = jnp.broadcast_to(plane[0, 0:1, :], (8, M))


def packed_edges(green):
    shapes = [jax.ShapeDtypeStruct((n, M), jnp.float32) for n in (SLOTS, 16, 8)]
    return pl.pallas_call(
        pack_edges,
        out_shape=shapes,
        grid=(1,),
        in_specs=[
            pl.BlockSpec((SLOTS, 8, M), lambda i: (1, 0, 0)),
            pl.BlockSpec((1, 16, M), lambda i: (0, 0, 0)),
        ],
        out_specs=[pl.BlockSpec(memory_space=pltpu.VMEM)] * 3,
        compiler_params=pltpu.CompilerParams(vmem_limit_bytes=16 * 1024 * 1024),
        cost_estimate=pl.CostEstimate(flops=10**6, bytes_accessed=10**6, transcendentals=0),
        name="pack_edges",
    )(green, green)


def exchange(value, axis):
    return lax.all_to_all(value, axis, split_axis=0, concat_axis=0, tiled=True)


def reflect(value, row_shift, col_shift):
    pairs = [
        (32 * r + j, 32 * ((row_shift - r) % 8) + (col_shift - j) % 32)
        for r in range(8)
        for j in range(32)
    ]
    return lax.ppermute(value, ("row", "col"), pairs)


def spread(value):
    value = jnp.where(lax.axis_index("row") == 0, value, 0.0)
    for step in (4, 2, 1):
        pairs = [(r, r + step) for r in range(0, 8, 2 * step)]
        value = value + lax.ppermute(value, "row", pairs)
    return value


def on_device(charge, green):
    z_table, forward, backward = (jnp.asarray(t) for t in tables())
    along_z = call(z_forward, (8, LANES, LANES), 60, charge.reshape(256, N), z_table)
    later, along_z = lax.optimization_barrier((green, along_z))
    moves = {
        "mirror": ("col", [(j, j ^ 29) for j in range(32)]),
        "across": (("row", "col"), [(i, i ^ 226) for i in range(256)]),
    }
    mirrors = []
    for k, order in enumerate((("mirror", "across"), ("across", "mirror"))):
        half = (green, later)[k][SLOTS:, 8 * k : 8 * (k + 1)]
        for name in order:
            half = lax.ppermute(half, *moves[name])
        mirrors.append(half)
    edge, plane, corner = packed_edges(green)
    mirror_edge = reflect(edge, 7, 32)
    start = reflect(plane, 8, 31)
    start_edge = reflect(corner, 8, 32)
    zero = spread(jnp.concatenate([plane, start, start_edge], 0))
    row = lax.axis_index("row")
    late = ((row >= 4).astype(jnp.int32) + (row == 4).astype(jnp.int32))[None]
    turned_up = call(
        turn_first, (3, M, LANES), 60, late, green, green, mirrors[0], start, zero,
        scalars=1, blocks=green_blocks(8, 1),
    )
    turned = call(
        turn_second, (5, M, LANES), 60, late, green, green, *mirrors, mirror_edge, start,
        start_edge, zero, scalars=1, blocks=green_blocks(16, 0),
    )
    by_rows = exchange(along_z, "row").reshape(1024, LANES)
    along_y = call(y_forward, (32, 8, 8, LANES), 16, by_rows, forward, scratch=[pltpu.VMEM((2 * M, LANES), jnp.float32)])
    by_cols = exchange(along_y.reshape(32, HALF, LANES), "col").reshape(2048, LANES)
    back_x = call(x_both, (2048, LANES), 24, by_cols, turned_up, turned, forward, backward)
    by_cells = exchange(back_x.reshape(32, HALF, LANES), "col")
    back_y = call(
        y_backward, (1024, LANES), 16, by_cells.reshape(32, 8, 8, LANES), backward,
        scratch=[pltpu.VMEM((2 * M, LANES), jnp.float32)],
    )
    by_parts = exchange(back_y.reshape(8, LANES, LANES), "row")
    back_z = call(z_backward, (256, N), 16, by_parts, z_table)
    return back_z.reshape(8, 32, N)


def solution(mesh):
    in_specs = (P("col", "row", None), P("row", "col", None))
    out_specs = P("col", "row", None)
    return jax.shard_map(
        on_device, mesh=mesh, in_specs=in_specs, out_specs=out_specs, check_vma=False
    )
```
